32 devices in a mesh: pose: 16 (over z, y, x), chan: 2 (over core).
Axes of the slice: x: 2, y: 2, z: 4, core: 2. Of those that a mesh axis runs over, the one named last changes fastest.
Arguments:
- atom_type: int32 [16, 2304], P('pose'), may hold values from 0 to 27
- occupancy: int32 [16, 2304], P('pose'), may hold values from 0 to 3
- atom_embed: bfloat16 [28, 128], replicated, may hold values from -6 to 6
- conv1_weight: bfloat16 [27, 128, 256], replicated, may hold values from -0.109375 to 0.109375
- conv1_bias: float32 [256], replicated, may hold values from -3 to 3
- conv2_weight: bfloat16 [27, 256, 128], replicated, may hold values from -0.078125 to 0.078125
- conv2_bias: float32 [128], replicated, may hold values from -3 to 3
- head_weight: float32 [128, 2304], P('chan'), may hold values from -0.0029296875 to 0.0029296875
Outputs:
- plane_scores: float32 [16], P('pose')
- scores: float32 [1], replicated
The draws below stay inside these ranges and needn't reach their ends.
All inputs are finite; a program needn't handle non-finite values.
Results may differ from the reference program's by a relative error of at most 0.0057.
Values may be sent and summed in bfloat16 or wider, within the bound.
No kernel may reach another device: no remote copies, remote signals or barrier semaphores. Data moves between devices by JAX's collectives and lax.ppermute only.
A program may use at most 64 MiB of HBM per device.

```python
import jax
import jax.numpy as jnp
from jax import lax

TYPES = 28
CIN = 128
MID = 256
COUT = 128
SIDE = 48
XPLANES = 16
PLANES = 1
POSES = 1


def set_ends(entries, key, smallest, largest):
    spot = [jax.random.randint(jax.random.fold_in(key, axis), (), 0, length) for axis, length in enumerate(entries.shape)]
    longest = entries.shape.index(max(entries.shape))
    beside = spot[:longest] + [(spot[longest] + 1) % entries.shape[longest]] + spot[longest + 1:]
    return entries.at[tuple(spot)].set(smallest).at[tuple(beside)].set(largest)


def shard_levels(own_key, extent, split, least, top_value):
    level, own = 1.0, jax.random.fold_in(own_key, 6)
    for dim, shards_of in split:
        draws = jnp.exp(jax.random.uniform(jax.random.fold_in(own, dim), (shards_of,), jnp.float32, least / len(split), top_value / len(split)))
        level = level * jnp.repeat(draws, extent[dim] // shards_of).reshape([-1 if axis == dim else 1 for axis in range(len(extent))])
    return level


def normal_values(key, extent, scale, bound, pieces=(), kind=jnp.bfloat16):
    result = scale * jax.random.normal(key, extent, jnp.float32)
    if pieces:
        result = result * shard_levels(key, extent, pieces, -0.22, 0.18)
    return jnp.clip(result, -bound, bound).astype(kind)


def setup_inputs(seed: int = 0) -> dict:
    keys = jax.random.split(jax.random.key(seed), 9)
    return {
        "atom_type": set_ends(jax.random.randint(keys[0], (POSES * XPLANES, SIDE * SIDE), 0, TYPES), jax.random.fold_in(keys[0], 1), 0, TYPES - 1).astype(jnp.int32),
        "occupancy": set_ends(jax.random.randint(keys[1], (POSES * XPLANES, SIDE * SIDE), 0, 4), jax.random.fold_in(keys[1], 1), 0, 3).astype(jnp.int32),
        "atom_embed": normal_values(keys[2], (TYPES, CIN), 1.0, 6.0),
        "conv1_weight": normal_values(keys[3], (27, CIN, MID), (27 * CIN) ** -0.5, 0.109375),
        "conv1_bias": normal_values(keys[4], (MID,), 0.5, 3.0, (), jnp.float32),
        "conv2_weight": normal_values(keys[5], (27, MID, COUT), (27 * MID) ** -0.5, 0.078125),
        "conv2_bias": normal_values(keys[6], (COUT,), 0.5, 3.0, (), jnp.float32),
        "head_weight": normal_values(keys[7], (COUT, SIDE * SIDE), (COUT * XPLANES * SIDE * SIDE) ** -0.5, 0.0029296875, ((0, 2),), jnp.float32),
    }


stencil_offsets = [(shift_x, shift_y, shift_z) for shift_x in (-1, 0, 1) for shift_y in (-1, 0, 1) for shift_z in (-1, 0, 1)]


def plane_shift(grid_field, shift_y, shift_z, grid_side):
    cell_count = grid_field.shape[-1]
    reach_cells = grid_side + 1
    flat_step = shift_y * grid_side + shift_z
    widths = [(0, 0)] * (grid_field.ndim - 1) + [(reach_cells, reach_cells)]
    padded = jnp.pad(grid_field, widths)
    shifted = lax.slice_in_dim(padded, reach_cells + flat_step, reach_cells + flat_step + cell_count, axis=grid_field.ndim - 1)
    positions = jnp.arange(cell_count, dtype=jnp.int32)
    coord_y = positions // grid_side + shift_y
    coord_z = positions % grid_side + shift_z
    inside = (coord_y >= 0) & (coord_y < grid_side) & (coord_z >= 0) & (coord_z < grid_side)
    return jnp.where(inside, shifted, jnp.zeros_like(shifted))


def convolve(padded, weight_taps, plane_count, grid_side):
    in_width = padded.shape[0]
    running = jnp.zeros((weight_taps.shape[2], plane_count * padded.shape[2]), jnp.float32)
    for offset_index, offset_item in enumerate(stencil_offsets):
        window = lax.slice_in_dim(padded, 1 + offset_item[0], 1 + offset_item[0] + plane_count, axis=1)
        shifted = plane_shift(window, offset_item[1], offset_item[2], grid_side).reshape(in_width, -1)
        running = running + jnp.dot(weight_taps[offset_index].T, shifted, preferred_element_type=jnp.float32)
    return running


def reorder_rows(grid_rows):
    block_count = XPLANES // PLANES
    parted = grid_rows.reshape(block_count, POSES, PLANES, SIDE * SIDE)
    return jnp.transpose(parted, (1, 0, 2, 3)).reshape(POSES, XPLANES, SIDE * SIDE)


def reference(atom_type, occupancy, atom_embed, conv1_weight, conv1_bias, conv2_weight, conv2_bias, head_weight):
    def score_pose(inputs):
        types, counts = inputs
        table = (types[None, :, :] == jnp.arange(TYPES, dtype=jnp.int32)[:, None, None]).astype(jnp.float32)
        features = (jnp.einsum("tc,txv->cxv", atom_embed.astype(jnp.float32), table) * counts.astype(jnp.float32)[None, :, :]).astype(jnp.bfloat16)
        padded = jnp.pad(features, ((0, 0), (1, 1), (0, 0)))
        hidden = jnp.maximum(convolve(padded, conv1_weight, XPLANES, SIDE) + conv1_bias[:, None], 0.0).astype(jnp.bfloat16)
        hidden = hidden.reshape(MID, XPLANES, SIDE * SIDE)
        padded_two = jnp.pad(hidden, ((0, 0), (1, 1), (0, 0)))
        mapped = jnp.maximum(convolve(padded_two, conv2_weight, XPLANES, SIDE) + conv2_bias[:, None], 0.0)
        mapped = mapped.reshape(COUT, XPLANES, SIDE * SIDE)
        return jnp.sum(mapped * head_weight[:, None, :], axis=(0, 2))

    planes = lax.map(score_pose, (reorder_rows(atom_type), reorder_rows(occupancy)))
    block_count = XPLANES // PLANES
    plane_rows = jnp.transpose(planes.reshape(POSES, block_count, PLANES), (1, 0, 2)).reshape(POSES * XPLANES)
    return plane_rows, jnp.sum(planes, axis=1)
```

```python
import functools

import jax
import jax.numpy as jnp
from jax import lax
from jax.experimental import pallas as pl
from jax.experimental.pallas import tpu as pltpu
from jax.sharding import PartitionSpec as P

SIDE = 48
XPLANES = 16
LANES = 128
TAPS = [(shift_y, shift_z) for shift_y in (-1, 0, 1) for shift_z in (-1, 0, 1)]

bf16 = jnp.bfloat16
f32 = jnp.float32
fp8 = jnp.float8_e4m3fn
REST_SCALE = 256.0


def fold_kernel(embed_ref, weight_ref, folded_ref, rest_ref, pair_ref, high_ref, low_ref):
    types = embed_ref.shape[0]
    embed = embed_ref[...].astype(f32)
    half = pair_ref.shape[0] // 2
    pair_ref[...] = jnp.zeros_like(pair_ref)
    pair_ref[:types, :] = embed
    pair_ref[half:half + types, :] = (3.0 * embed).astype(bf16).astype(f32)
    pair = pair_ref[...].astype(bf16)
    high_ref[...] = jnp.zeros_like(high_ref)
    low_ref[...] = jnp.zeros_like(low_ref)
    for dx in range(3):
        for tap in range(9):
            both = jnp.dot(pair, weight_ref[dx * 9 + tap], preferred_element_type=f32)
            once, thrice = both[:types, :], both[half:half + types, :]
            rounded = once.astype(bf16).astype(f32)
            first = 2 * types * tap
            high_ref[dx, types * tap:types * (tap + 1), :] = rounded
            low_ref[dx, first:first + types, :] = once - rounded
            low_ref[dx, first + types:first + 2 * types, :] = thrice - 3.0 * rounded
        folded_ref[dx] = high_ref[dx].astype(bf16)
        rest_ref[dx] = (low_ref[dx] * REST_SCALE).astype(fp8)


def fold_embedding(atom_embed, conv1_weight):
    types, width = atom_embed.shape
    mid = conv1_weight.shape[2]
    depth = round_up(9 * types, LANES)
    rest_depth = round_up(18 * types, LANES)
    return pl.pallas_call(
        fold_kernel,
        out_shape=(
            jax.ShapeDtypeStruct((3, depth, mid), bf16),
            jax.ShapeDtypeStruct((3, rest_depth, mid), fp8),
        ),
        scratch_shapes=[
            pltpu.VMEM((2 * round_up(types, 16), width), f32),
            pltpu.VMEM((3, depth, mid), f32),
            pltpu.VMEM((3, rest_depth, mid), f32),
        ],
        name="fold_embedding",
    )(atom_embed, conv1_weight)


def round_up(value, step):
    return -(-value // step) * step


def one_hot(rows, x, types, depth):
    width = rows[0][0].shape[1]
    sub = lax.broadcasted_iota(jnp.int32, (8, 1), 0)

    def spread(row):
        return jnp.broadcast_to(row[x:x + 1, :], (8, width))

    groups = []
    for first in range(0, depth, 8):
        low, high = first // types, (first + 7) // types
        if low >= len(rows):
            groups.append(jnp.zeros((8, width), f32))
            continue
        kind, count = spread(rows[low][0]), spread(rows[low][1])
        number = sub + (first - types * low)
        if high != low:
            own = sub < types * high - first
            number = jnp.where(own, number, number - types)
            if high < len(rows):
                kind = jnp.where(own, kind, spread(rows[high][0]))
                count = jnp.where(own, count, spread(rows[high][1]))
            else:
                count = jnp.where(own, count, 0.0)
        groups.append(jnp.where(kind == number, count, 0.0))
    return jnp.concatenate(groups, axis=0)


def main_kernel(
    chunk,
    pose_total,
    group_size,
    own_ref,
    near_ref,
    far_ref,
    head_own_hbm,
    head_far_hbm,
    folded_ref,
    rest_ref,
    bias1_ref,
    weight2_ref,
    bias2_ref,
    out_ref,
    planes_ref,
    onehot_ref,
    resthot_ref,
    hidden_ref,
    taps_ref,
    w2_ref,
    head_ref,
    sems,
):
    w2_copy = pltpu.make_async_copy(weight2_ref, w2_ref, sems.at[0])
    w2_copy.start()
    chan = lax.axis_index("chan")
    share = head_own_hbm.shape[0]
    head_cells = pl.ds(pl.multiple_of(chan * head_ref.shape[1], LANES), head_ref.shape[1])
    head_copies = [
        pltpu.make_async_copy(
            source.at[:, head_cells],
            head_ref.at[pl.ds(pl.multiple_of(part * share, share), share), :],
            sems.at[1 + number],
        )
        for number, (source, part) in enumerate(((head_own_hbm, chan), (head_far_hbm, 1 - chan)))
    ]
    for copy in head_copies:
        copy.start()
    block = lax.axis_index("pose") // pose_total
    plane_cells = own_ref.shape[1]
    half_cells = plane_cells // 2
    depth = folded_ref.shape[1]
    padded = hidden_ref.shape[1]
    types = 28
    window = half_cells + 3 * LANES

    planes_ref[...] = jnp.zeros_like(planes_ref)
    near, far = near_ref[...], far_ref[...]
    below = jnp.where(chan == 1, near, far)
    above = jnp.where(chan == 1, far, near)
    rows = [
        jnp.where(block >= 2, below[:, plane_cells:], 0),
        jnp.where(block >= 1, below[:, :plane_cells], 0),
        own_ref[...],
        jnp.where(block <= group_size - 2, above[:, :plane_cells], 0),
        jnp.where(block <= group_size - 3, above[:, plane_cells:], 0),
    ]
    for x in range(5):
        planes_ref[x:x + 1, LANES:LANES + plane_cells] = rows[x]
    start = pl.multiple_of(chan * half_cells, LANES)
    cells = planes_ref[:, pl.ds(start, window)]

    column = lax.rem(lax.broadcasted_iota(jnp.int32, (8, padded), 1), SIDE)
    plain, split = [], []
    for shift_y, shift_z in TAPS:
        first = LANES - SIDE + SIDE * shift_y + shift_z
        moved = cells[:, first:first + padded]
        inside = (column + shift_z >= 0) & (column + shift_z < SIDE)
        moved = jnp.where(inside, moved, 0)
        kind = lax.shift_right_logical(moved, 2)
        count = moved & 3
        plain.append((kind, count.astype(f32)))
        split.append(
            (
                jnp.where(count == 3, kind + types, kind),
                jnp.where(count == 3, 1, count).astype(f32),
            )
        )
    for x in range(5):
        onehot_ref[x] = one_hot(plain, x, types, depth).astype(bf16).T
        resthot_ref[x] = one_hot(split, x, 2 * types, rest_ref.shape[1]).astype(bf16).T.astype(fp8)

    bias1 = bias1_ref[...]
    for h in range(3):
        plane_ok = (block + (h - 1) >= 0) & (block + (h - 1) < group_size)
        for first in range(0, padded, chunk):
            total, rest = bias1, 0.0
            for dx in range(3):
                rest = rest + jnp.dot(
                    resthot_ref[h + dx, first:first + chunk, :],
                    rest_ref[dx],
                    preferred_element_type=f32,
                )
                total = total + jnp.dot(
                    onehot_ref[h + dx, first:first + chunk, :],
                    folded_ref[dx],
                    preferred_element_type=f32,
                )
            total = total + rest * (1.0 / REST_SCALE)
            index = first + lax.broadcasted_iota(jnp.int32, (chunk, 1), 0)
            lowest = jnp.where(plane_ok, jnp.where(chan == 0, SIDE, 0), padded)
            highest = jnp.where(chan == 0, half_cells + 2 * SIDE, half_cells + SIDE)
            inside = (index >= lowest) & (index < highest)
            hidden_ref[h, first:first + chunk, :] = jnp.where(
                inside, jnp.maximum(total, 0.0), 0.0
            ).astype(bf16)

    w2_copy.wait()
    out_width = weight2_ref.shape[2]
    for first in range(0, padded, chunk):
        total = None
        for h in range(3):
            taps = jnp.concatenate([w2_ref[h * 9 + tap] for tap in range(9)], axis=1)
            part = jnp.dot(
                hidden_ref[h, first:first + chunk, :], taps, preferred_element_type=f32
            )
            total = part if total is None else total + part
        for tap in range(9):
            taps_ref[tap, 8 + first:8 + first + chunk, :] = total[
                :, tap * out_width:(tap + 1) * out_width
            ]

    for copy in head_copies:
        copy.wait()
    bias2 = bias2_ref[...]
    running = jnp.zeros((8, out_width), f32)
    for first in range(0, half_cells, LANES):
        moved = []
        for shift_z in range(3):
            offset = 8 + first + shift_z - 1
            moved.append(
                taps_ref[shift_z, offset:offset + LANES, :]
                + taps_ref[3 + shift_z, offset + SIDE:offset + SIDE + LANES, :]
                + taps_ref[6 + shift_z, offset + 2 * SIDE:offset + 2 * SIDE + LANES, :]
            )
        column = lax.rem(first + lax.broadcasted_iota(jnp.int32, (LANES, 1), 0), SIDE)
        mapped = (
            bias2
            + moved[1]
            + jnp.where(column > 0, moved[0], 0.0)
            + jnp.where(column < SIDE - 1, moved[2], 0.0)
        )
        mapped = jnp.maximum(mapped, 0.0)
        scored = mapped * head_ref[:, first:first + LANES].T
        running = running + jnp.sum(scored.reshape(LANES // 8, 8, out_width), axis=0)
    out_ref[...] = jnp.broadcast_to(jnp.sum(running), out_ref.shape)


def rescore(own, near, far, head_own, head_far, folded, rest, bias1, weight2, bias2, copies):
    plane_cells = own.shape[1]
    half_cells = plane_cells // 2
    depth, mid = folded.shape[1:]
    width = weight2.shape[2]
    chunk = 256
    padded = round_up(half_cells + 2 * SIDE, chunk)
    pose_total = lax.axis_size("pose") // XPLANES
    vmem = pl.BlockSpec(memory_space=pltpu.VMEM)
    hbm = pl.BlockSpec(memory_space=pl.ANY)
    return pl.pallas_call(
        functools.partial(main_kernel, chunk, pose_total, XPLANES),
        out_shape=jax.ShapeDtypeStruct((copies, LANES), f32),
        in_specs=[vmem] * 3 + [hbm] * 2 + [vmem] * 3 + [hbm, vmem],
        out_specs=vmem,
        scratch_shapes=[
            pltpu.VMEM((8, plane_cells + 3 * LANES), jnp.int32),
            pltpu.VMEM((5, padded, depth), bf16),
            pltpu.VMEM((5, padded, rest.shape[1]), fp8),
            pltpu.VMEM((3, padded, mid), bf16),
            pltpu.VMEM((9, padded + 16, width), f32),
            pltpu.VMEM(weight2.shape, bf16),
            pltpu.VMEM((width, half_cells), f32),
            pltpu.SemaphoreType.DMA((3,)),
        ],
        name="rescore",
    )(own, near, far, head_own, head_far, folded, rest, bias1, weight2, bias2)


def final_kernel(pose_total, chan_count, parts_ref, plane_ref, scores_ref):
    parts = parts_ref[:, 0, :]
    pose = lax.broadcasted_iota(jnp.int32, parts.shape, 0) // chan_count
    first = lax.broadcasted_iota(jnp.int32, parts.shape, 1) == 0
    plane_ref[0] = jnp.sum(jnp.where(first & (pose == lax.axis_index("pose")), parts, 0.0))
    for p in range(pose_total):
        scores_ref[p] = jnp.sum(jnp.where(first & (lax.rem(pose, pose_total) == p), parts, 0.0))


def final_sums(parts, pose_total, chan_count):
    smem = pl.BlockSpec(memory_space=pltpu.SMEM)
    return pl.pallas_call(
        functools.partial(final_kernel, pose_total, chan_count),
        out_shape=(
            jax.ShapeDtypeStruct((1,), f32),
            jax.ShapeDtypeStruct((pose_total,), f32),
        ),
        out_specs=(smem, smem),
        name="final_sums",
    )(parts)


def on_device(
    atom_type,
    occupancy,
    atom_embed,
    conv1_weight,
    conv1_bias,
    conv2_weight,
    conv2_bias,
    head_weight,
):
    chan_count = lax.axis_size("chan")
    pose_count = lax.axis_size("pose")
    pose_total = pose_count // XPLANES
    swap = [(0, 1), (1, 0)]

    def fetch(steps):
        by = steps * pose_total
        pairs = []
        for i in range(pose_count):
            up = 2 * (i + by) + 1 if i + by < pose_count else 2 * i
            down = 2 * (i - by) if i >= by else 2 * i + 1
            pairs += [(2 * i, down), (2 * i + 1, up)]
        return lax.ppermute(code, ("pose", "chan"), pairs)

    code = atom_type * 4 + occupancy
    near = jnp.concatenate([fetch(1), fetch(2)], axis=1)
    folded, rest = fold_embedding(atom_embed, conv1_weight)
    far = lax.ppermute(near, "chan", swap)
    head_far = lax.ppermute(head_weight, "chan", swap)
    part = rescore(
        code,
        near,
        far,
        head_weight,
        head_far,
        folded,
        rest,
        conv1_bias[None, :],
        conv2_weight,
        conv2_bias[None, :],
        pose_count * chan_count,
    )
    parts = lax.all_to_all(part[:, None, :], ("pose", "chan"), 0, 0, tiled=True)
    return final_sums(parts, pose_total, chan_count)


def solution(mesh):
    return jax.shard_map(
        on_device,
        mesh=mesh,
        in_specs=(P("pose", None), P("pose", None), P(), P(), P(), P(), P(), P("chan", None)),
        out_specs=(P("pose"), P()),
        check_vma=False,
    )
```

```python
import functools

import jax
import jax.numpy as jnp
from jax import lax
from jax.experimental import pallas as pl
from jax.experimental.pallas import tpu as pltpu
from jax.sharding import PartitionSpec as P

SIDE = 48
XPLANES = 16
LANES = 128
TILE = 256
CHUNK = 256
TAPS = [(shift_y, shift_z) for shift_y in (-1, 0, 1) for shift_z in (-1, 0, 1)]

bf16 = jnp.bfloat16
f32 = jnp.float32


def in_vmem(array):
    return pltpu.with_memory_space_constraint(array, pltpu.VMEM)


def fold_kernel(embed_ref, weight_ref, folded_ref, pair_ref, rows_ref):
    types = embed_ref.shape[0]
    embed = embed_ref[...].astype(f32)
    half = pair_ref.shape[0] // 2
    rest = round_up(9 * types, LANES)
    pair_ref[...] = jnp.zeros_like(pair_ref)
    pair_ref[:types, :] = embed
    pair_ref[half:half + types, :] = (3.0 * embed).astype(bf16).astype(f32)
    pair = pair_ref[...].astype(bf16)
    rows_ref[...] = jnp.zeros_like(rows_ref)
    for dx in range(3):
        for tap in range(9):
            both = jnp.dot(pair, weight_ref[dx * 9 + tap], preferred_element_type=f32)
            once, thrice = both[:types, :], both[half:half + types, :]
            rounded = once.astype(bf16).astype(f32)
            first = rest + 2 * types * tap
            rows_ref[dx, types * tap:types * (tap + 1), :] = rounded
            rows_ref[dx, first:first + types, :] = once - rounded
            rows_ref[dx, first + types:first + 2 * types, :] = thrice - 3.0 * rounded
        folded_ref[dx] = rows_ref[dx].astype(bf16)


def fold_embedding(atom_embed, conv1_weight):
    types, width = atom_embed.shape
    mid = conv1_weight.shape[2]
    depth = round_up(9 * types, LANES) + round_up(18 * types, LANES)
    return pl.pallas_call(
        fold_kernel,
        out_shape=pltpu.VMEM((3, depth, mid), bf16),
        scratch_shapes=[
            pltpu.VMEM((2 * round_up(types, 16), width), f32),
            pltpu.VMEM((3, depth, mid), f32),
        ],
        compiler_params=pltpu.CompilerParams(vmem_limit_bytes=12 << 20),
        name="fold_embedding",
    )(atom_embed, in_vmem(conv1_weight))


def round_up(value, step):
    return -(-value // step) * step


def one_hot(rows, x, types, start):
    width = TILE
    depth = round_up(types * len(rows), LANES)
    sub = lax.broadcasted_iota(jnp.int32, (8, 1), 0)

    def spread(row):
        return jnp.broadcast_to(row[x:x + 1, start:start + width], (8, width))

    groups = []
    for first in range(0, depth, 8):
        low, high = first // types, (first + 7) // types
        if low >= len(rows):
            groups.append(jnp.zeros((8, width), f32))
            continue
        kind, count = spread(rows[low][0]), spread(rows[low][1])
        number = sub + (first - types * low)
        if high != low:
            own = sub < types * high - first
            number = jnp.where(own, number, number - types)
            if high < len(rows):
                kind = jnp.where(own, kind, spread(rows[high][0]))
                count = jnp.where(own, count, spread(rows[high][1]))
            else:
                count = jnp.where(own, count, 0.0)
        groups.append(jnp.where(kind == number, count, 0.0))
    return jnp.concatenate(groups, axis=0)


def main_kernel(
    chunk,
    pose_total,
    group_size,
    own_ref,
    near_ref,
    far_ref,
    head_own_ref,
    head_far_ref,
    folded_ref,
    bias1_ref,
    weight2_ref,
    bias2_ref,
    out_ref,
    planes_ref,
    onehot_ref,
    hidden_ref,
    taps_ref,
    head_ref,
):
    chan = lax.axis_index("chan")
    block = lax.axis_index("pose") // pose_total
    plane_cells = own_ref.shape[1]
    half_cells = plane_cells // 2
    padded = hidden_ref.shape[1]
    types = 28
    window = half_cells + 3 * LANES

    planes_ref[...] = jnp.zeros_like(planes_ref)
    near, far = near_ref[...], far_ref[...]
    below = jnp.where(chan == 1, near, far)
    above = jnp.where(chan == 1, far, near)
    rows = [
        jnp.where(block >= 2, below[:, plane_cells:], 0),
        jnp.where(block >= 1, below[:, :plane_cells], 0),
        own_ref[...],
        jnp.where(block <= group_size - 2, above[:, :plane_cells], 0),
        jnp.where(block <= group_size - 3, above[:, plane_cells:], 0),
    ]
    for x in range(5):
        planes_ref[x:x + 1, LANES:LANES + plane_cells] = rows[x]
    start = pl.multiple_of(chan * half_cells, LANES)
    cells = planes_ref[:, pl.ds(start, window)]

    column = lax.rem(lax.broadcasted_iota(jnp.int32, (8, padded), 1), SIDE)
    plain, split = [], []
    for shift_y, shift_z in TAPS:
        first = LANES - SIDE + SIDE * shift_y + shift_z
        moved = cells[:, first:first + padded]
        inside = (column + shift_z >= 0) & (column + shift_z < SIDE)
        moved = jnp.where(inside, moved, 0)
        kind = lax.shift_right_logical(moved, 2)
        count = moved & 3
        plain.append((kind, count.astype(f32)))
        split.append(
            (
                jnp.where(count == 3, kind + types, kind),
                jnp.where(count == 3, 1, count).astype(f32),
            )
        )
    bias1 = bias1_ref[...]
    for first in range(0, padded, TILE):
        for x in range(5):
            onehot_ref[x, first:first + TILE, :] = jnp.concatenate(
                [
                    one_hot(plain, x, types, first),
                    one_hot(split, x, 2 * types, first),
                ],
                axis=0,
            ).astype(bf16).T
    for first in range(0, padded, chunk):
        for h in range(3):
            plane_ok = (block + (h - 1) >= 0) & (block + (h - 1) < group_size)
            total = bias1
            for dx in range(3):
                total = total + jnp.dot(
                    onehot_ref[h + dx, first:first + chunk, :],
                    folded_ref[dx],
                    preferred_element_type=f32,
                )
            index = first + lax.broadcasted_iota(jnp.int32, (chunk, 1), 0)
            lowest = jnp.where(plane_ok, jnp.where(chan == 0, SIDE, 0), padded)
            highest = jnp.where(chan == 0, half_cells + 2 * SIDE, half_cells + SIDE)
            inside = (index >= lowest) & (index < highest)
            hidden_ref[h, first:first + chunk, :] = jnp.where(
                inside, jnp.maximum(total, 0.0), 0.0
            ).astype(bf16)

    out_width = weight2_ref.shape[2]
    for first in range(0, padded, chunk):
        total = None
        for h in range(3):
            taps = jnp.concatenate([weight2_ref[h * 9 + tap] for tap in range(9)], axis=1)
            part = jnp.dot(
                hidden_ref[h, first:first + chunk, :], taps, preferred_element_type=f32
            )
            total = part if total is None else total + part
        for tap in range(9):
            taps_ref[tap, 8 + first:8 + first + chunk, :] = total[
                :, tap * out_width:(tap + 1) * out_width
            ]

    share = head_own_ref.shape[0]
    head_cells = pl.ds(start, half_cells)
    head_ref[pl.ds(pl.multiple_of(chan * share, share), share), :] = head_own_ref[:, head_cells]
    head_ref[pl.ds(pl.multiple_of((1 - chan) * share, share), share), :] = head_far_ref[
        :, head_cells
    ]
    bias2 = bias2_ref[...]
    running = jnp.zeros((8, out_width), f32)
    for first in range(0, half_cells, LANES):
        moved = []
        for shift_z in range(3):
            offset = 8 + first + shift_z - 1
            moved.append(
                taps_ref[shift_z, offset:offset + LANES, :]
                + taps_ref[3 + shift_z, offset + SIDE:offset + SIDE + LANES, :]
                + taps_ref[6 + shift_z, offset + 2 * SIDE:offset + 2 * SIDE + LANES, :]
            )
        column = lax.rem(first + lax.broadcasted_iota(jnp.int32, (LANES, 1), 0), SIDE)
        mapped = (
            bias2
            + moved[1]
            + jnp.where(column > 0, moved[0], 0.0)
            + jnp.where(column < SIDE - 1, moved[2], 0.0)
        )
        mapped = jnp.maximum(mapped, 0.0)
        scored = mapped * head_ref[:, first:first + LANES].T
        running = running + jnp.sum(scored.reshape(LANES // 8, 8, out_width), axis=0)
    out_ref[...] = jnp.broadcast_to(jnp.sum(running), out_ref.shape)


def rescore(own, near, far, head_own, head_far, folded, bias1, weight2, bias2, copies):
    plane_cells = own.shape[1]
    half_cells = plane_cells // 2
    depth, mid = folded.shape[1:]
    width = weight2.shape[2]
    chunk = CHUNK
    padded = round_up(half_cells + 2 * SIDE, TILE)
    pose_total = lax.axis_size("pose") // XPLANES
    vmem = pl.BlockSpec(memory_space=pltpu.VMEM)
    return pl.pallas_call(
        functools.partial(main_kernel, chunk, pose_total, XPLANES),
        out_shape=pltpu.VMEM((copies, LANES), f32),
        in_specs=[vmem] * 9,
        out_specs=vmem,
        scratch_shapes=[
            pltpu.VMEM((8, plane_cells + 3 * LANES), jnp.int32),
            pltpu.VMEM((5, padded, depth), bf16),
            pltpu.VMEM((3, padded, mid), bf16),
            pltpu.VMEM((9, padded + 16, width), f32),
            pltpu.VMEM((width, half_cells), f32),
        ],
        compiler_params=pltpu.CompilerParams(vmem_limit_bytes=40 << 20),
        name="rescore",
    )(
        in_vmem(own),
        in_vmem(near),
        in_vmem(far),
        in_vmem(head_own),
        in_vmem(head_far),
        in_vmem(folded),
        bias1,
        in_vmem(weight2),
        bias2,
    )


def final_kernel(pose_total, chan_count, parts_ref, plane_ref, scores_ref):
    parts = parts_ref[:, 0, :]
    pose = lax.broadcasted_iota(jnp.int32, parts.shape, 0) // chan_count
    first = lax.broadcasted_iota(jnp.int32, parts.shape, 1) == 0
    plane_ref[0] = jnp.sum(jnp.where(first & (pose == lax.axis_index("pose")), parts, 0.0))
    for p in range(pose_total):
        scores_ref[p] = jnp.sum(jnp.where(first & (lax.rem(pose, pose_total) == p), parts, 0.0))


def final_sums(parts, pose_total, chan_count):
    smem = pl.BlockSpec(memory_space=pltpu.SMEM)
    return pl.pallas_call(
        functools.partial(final_kernel, pose_total, chan_count),
        out_shape=(
            jax.ShapeDtypeStruct((1,), f32),
            jax.ShapeDtypeStruct((pose_total,), f32),
        ),
        out_specs=(smem, smem),
        compiler_params=pltpu.CompilerParams(vmem_limit_bytes=1 << 20),
        name="final_sums",
    )(in_vmem(parts))


def on_device(
    atom_type,
    occupancy,
    atom_embed,
    conv1_weight,
    conv1_bias,
    conv2_weight,
    conv2_bias,
    head_weight,
):
    chan_count = lax.axis_size("chan")
    pose_count = lax.axis_size("pose")
    pose_total = pose_count // XPLANES
    swap = [(0, 1), (1, 0)]

    def fetch(steps):
        by = steps * pose_total
        pairs = []
        for i in range(pose_count):
            up = 2 * (i + by) + 1 if i + by < pose_count else 2 * i
            down = 2 * (i - by) if i >= by else 2 * i + 1
            pairs += [(2 * i, down), (2 * i + 1, up)]
        return lax.ppermute(code, ("pose", "chan"), pairs)

    code = atom_type * 4 + occupancy
    first, second, folded = lax.optimization_barrier(
        (fetch(1), fetch(2), fold_embedding(atom_embed, conv1_weight))
    )
    near = jnp.concatenate([first, second], axis=1)
    far = lax.ppermute(near, "chan", swap)
    head_far = lax.ppermute(head_weight, "chan", swap)
    part = rescore(
        code,
        near,
        far,
        head_weight,
        head_far,
        folded,
        conv1_bias[None, :],
        conv2_weight,
        conv2_bias[None, :],
        pose_count * chan_count,
    )
    parts = lax.all_to_all(part[:, None, :], ("pose", "chan"), 0, 0, tiled=True)
    return final_sums(parts, pose_total, chan_count)


def solution(mesh):
    return jax.shard_map(
        on_device,
        mesh=mesh,
        in_specs=(P("pose", None), P("pose", None), P(), P(), P(), P(), P(), P("chan", None)),
        out_specs=(P("pose"), P()),
        check_vma=False,
    )
```

```python
import functools

import jax
import jax.numpy as jnp
from jax import lax
from jax.experimental import pallas as pl
from jax.experimental.pallas import tpu as pltpu
from jax.sharding import PartitionSpec as P

SIDE = 48
XPLANES = 16
LANES = 128
TILE = 256
PARTS = 3
TAPS = [(shift_y, shift_z) for shift_y in (-1, 0, 1) for shift_z in (-1, 0, 1)]

bf16 = jnp.bfloat16
f32 = jnp.float32


def in_vmem(array):
    return pltpu.with_memory_space_constraint(array, pltpu.VMEM)


def in_hbm(array):
    return pltpu.with_memory_space_constraint(array, pltpu.HBM)


def round_up(value, step):
    return -(-value // step) * step


def params(megabytes):
    return pltpu.CompilerParams(vmem_limit_bytes=megabytes << 20)


def encode_kernel(type_hbm, count_hbm, embed_hbm, code_ref, pair_ref, type_ref, count_ref, embed_ref, sems):
    types = embed_ref.shape[0]
    half = pair_ref.shape[0] // 2
    copies = [
        pltpu.make_async_copy(source, target, sems.at[n])
        for n, (source, target) in enumerate(
            ((type_hbm, type_ref), (count_hbm, count_ref), (embed_hbm, embed_ref))
        )
    ]
    for copy in copies:
        copy.start()
    pair_ref[...] = jnp.zeros_like(pair_ref)
    for copy in copies:
        copy.wait()
    code_ref[...] = type_ref[...] * 4 + count_ref[...]
    embed = embed_ref[...].astype(f32)
    pair_ref[:types, :] = embed
    pair_ref[half:half + types, :] = (3.0 * embed).astype(bf16).astype(f32)


def encode(atom_type, occupancy, atom_embed):
    types, width = atom_embed.shape
    return pl.pallas_call(
        encode_kernel,
        out_shape=(
            pltpu.VMEM(atom_type.shape, jnp.int32),
            pltpu.VMEM((2 * round_up(types, 16), width), f32),
        ),
        in_specs=[pl.BlockSpec(memory_space=pl.ANY)] * 3,
        scratch_shapes=[
            pltpu.VMEM(atom_type.shape, jnp.int32),
            pltpu.VMEM(atom_type.shape, jnp.int32),
            pltpu.VMEM(atom_embed.shape, bf16),
            pltpu.SemaphoreType.DMA((3,)),
        ],
        compiler_params=params(1),
        name="encode",
    )(in_hbm(atom_type), in_hbm(occupancy), in_hbm(atom_embed))


def fold_kernel(types, pair_ref, weight_ref, folded_ref, rows_ref):
    half = pair_ref.shape[0] // 2
    rest = round_up(9 * types, LANES)
    pair = pair_ref[...].astype(bf16)
    rows_ref[...] = jnp.zeros_like(rows_ref)
    for dx in range(3):
        for tap in range(9):
            both = jnp.dot(pair, weight_ref[dx * 9 + tap], preferred_element_type=f32)
            once, thrice = both[:types, :], both[half:half + types, :]
            rounded = once.astype(bf16).astype(f32)
            first = rest + 2 * types * tap
            rows_ref[dx, types * tap:types * (tap + 1), :] = rounded
            rows_ref[dx, first:first + types, :] = once - rounded
            rows_ref[dx, first + types:first + 2 * types, :] = thrice - 3.0 * rounded
        folded_ref[dx] = rows_ref[dx].astype(bf16)


def fold_embedding(types, pair, conv1_weight):
    mid = conv1_weight.shape[2]
    depth = round_up(9 * types, LANES) + round_up(18 * types, LANES)
    return pl.pallas_call(
        functools.partial(fold_kernel, types),
        out_shape=pltpu.VMEM((3, depth, mid), bf16),
        scratch_shapes=[pltpu.VMEM((3, depth, mid), f32)],
        compiler_params=params(12),
        name="fold_embedding",
    )(in_vmem(pair), in_vmem(conv1_weight))


def one_hot(rows, x, types, start):
    width = TILE
    depth = round_up(types * len(rows), LANES)
    sub = lax.broadcasted_iota(jnp.int32, (8, 1), 0)

    def spread(row):
        return jnp.broadcast_to(row[x:x + 1, start:start + width], (8, width))

    groups = []
    for first in range(0, depth, 8):
        low, high = first // types, (first + 7) // types
        if low >= len(rows):
            groups.append(jnp.zeros((8, width), f32))
            continue
        kind, count = spread(rows[low][0]), spread(rows[low][1])
        number = sub + (first - types * low)
        if high != low:
            own = sub < types * high - first
            number = jnp.where(own, number, number - types)
            if high < len(rows):
                kind = jnp.where(own, kind, spread(rows[high][0]))
                count = jnp.where(own, count, spread(rows[high][1]))
            else:
                count = jnp.where(own, count, 0.0)
        groups.append(jnp.where(kind == number, count, 0.0))
    return jnp.concatenate(groups, axis=0)


def position(pose_total):
    chan = lax.axis_index("chan")
    block = lax.axis_index("pose") // pose_total
    behind = jnp.where(chan == 1, block, XPLANES - 1 - block)
    return chan, behind, [jnp.where(chan == 1, dx, 2 - dx) for dx in range(3)]


def tap_rows(planes_ref, rows, chan, padded, types):
    plane_cells = rows[0].shape[1]
    half_cells = plane_cells // 2
    planes_ref[...] = jnp.zeros_like(planes_ref)
    for x, row in enumerate(rows):
        planes_ref[x:x + 1, LANES:LANES + plane_cells] = row
    start = pl.multiple_of(chan * half_cells, LANES)
    cells = planes_ref[:, pl.ds(start, half_cells + 3 * LANES)]
    column = lax.rem(lax.broadcasted_iota(jnp.int32, (8, padded), 1), SIDE)
    plain, split = [], []
    for shift_y, shift_z in TAPS:
        first = LANES - SIDE + SIDE * shift_y + shift_z
        moved = cells[:, first:first + padded]
        inside = (column + shift_z >= 0) & (column + shift_z < SIDE)
        moved = jnp.where(inside, moved, 0)
        kind = lax.shift_right_logical(moved, 2)
        count = moved & 3
        plain.append((kind, count.astype(f32)))
        split.append(
            (
                jnp.where(count == 3, kind + types, kind),
                jnp.where(count == 3, 1, count).astype(f32),
            )
        )
    return plain, split


def both_hot(plain, split, x, types, first):
    return jnp.concatenate(
        [one_hot(plain, x, types, first), one_hot(split, x, 2 * types, first)], axis=0
    ).astype(bf16).T


def hidden_rows(operands, bias1, folded_ref, order, first, size, half_cells, chan, plane_ok):
    total = bias1
    for dx in range(3):
        total = total + jnp.dot(
            operands[dx](first, size), folded_ref[order[dx]], preferred_element_type=f32
        )
    index = first + lax.broadcasted_iota(jnp.int32, (size, 1), 0)
    lowest = jnp.where(plane_ok, jnp.where(chan == 0, SIDE, 0), half_cells + 2 * SIDE)
    highest = jnp.where(chan == 0, half_cells + 2 * SIDE, half_cells + SIDE)
    inside = (index >= lowest) & (index < highest)
    return jnp.where(inside, jnp.maximum(total, 0.0), 0.0).astype(bf16)


def reader(ref, x):
    return lambda first, size: ref[x, first:first + size, :]


def score_kernel(
    pose_total,
    types,
    own_ref,
    near_ref,
    far_ref,
    head_own_ref,
    head_far_ref,
    folded_ref,
    bias1_ref,
    weight2_ref,
    bias2_ref,
    out_ref,
    planes_ref,
    hot_ref,
    hidden_ref,
    sums_ref,
    head_ref,
):
    chan, behind, order = position(pose_total)
    plane_cells = own_ref.shape[1]
    half_cells = plane_cells // 2
    padded = hot_ref.shape[1]
    used = half_cells + 2 * SIDE
    share = head_own_ref.shape[0]
    head_cells = pl.ds(pl.multiple_of(chan * half_cells, LANES), half_cells)
    head_ref[pl.ds(pl.multiple_of(chan * share, share), share), :] = head_own_ref[:, head_cells]
    head_ref[pl.ds(pl.multiple_of((1 - chan) * share, share), share), :] = head_far_ref[
        :, head_cells
    ]
    near, far = near_ref[...], far_ref[...]
    rows = [
        jnp.where(behind >= 2, near[:, plane_cells:], 0),
        jnp.where(behind >= 1, near[:, :plane_cells], 0),
        own_ref[...],
        jnp.where(behind <= XPLANES - 2, far[:, :plane_cells], 0),
        jnp.where(behind <= XPLANES - 3, far[:, plane_cells:], 0),
    ]
    plain, split = tap_rows(planes_ref, rows, chan, padded, types)
    bias1 = bias1_ref[...]
    operands = [reader(hot_ref, x) for x in range(5)]
    plane_ok = [behind >= 1, True, behind <= XPLANES - 2]
    for first in range(0, padded, TILE):
        size = min(TILE, used - first)
        for x in range(5):
            hot_ref[x, first:first + TILE, :] = both_hot(plain, split, x, types, first)
            if x >= 2:
                h = x - 2
                hidden_ref[h, first:first + size, :] = hidden_rows(
                    operands[h:], bias1, folded_ref, order, first, size, half_cells, chan, plane_ok[h]
                )

    width = weight2_ref.shape[2]
    hidden = [reader(hidden_ref, h) for h in range(3)]

    def taps(first, size, *numbers):
        total = None
        for h in range(3):
            weights = [weight2_ref[order[h] * 9 + tap] for tap in numbers]
            part = jnp.dot(
                hidden[h](first, size),
                jnp.concatenate(weights, axis=1),
                preferred_element_type=f32,
            )
            total = part if total is None else total + part
        return [total[:, n * width:(n + 1) * width] for n in range(len(numbers))]

    ends = [(0, half_cells), (0, half_cells + SIDE), (SIDE, half_cells + SIDE), (2 * SIDE, used), (2 * SIDE, used)]
    for pair, (begin, end) in enumerate(ends):
        size = (end - begin) // PARTS
        numbers = [2 * pair, 2 * pair + 1][: 2 if pair < 4 else 1]
        for first in range(begin, end, size):
            for number, value in zip(numbers, taps(first, size, *numbers)):
                sums_ref[number, 8 + first:8 + first + size, :] = value
    bias2 = bias2_ref[...]
    running = jnp.zeros((8, width), f32)
    for first in range(0, half_cells, LANES):
        moved = []
        for shift_z in range(3):
            offset = 8 + first + shift_z - 1
            moved.append(
                sums_ref[shift_z, offset:offset + LANES, :]
                + sums_ref[3 + shift_z, offset + SIDE:offset + SIDE + LANES, :]
                + sums_ref[6 + shift_z, offset + 2 * SIDE:offset + 2 * SIDE + LANES, :]
            )
        column = lax.rem(first + lax.broadcasted_iota(jnp.int32, (LANES, 1), 0), SIDE)
        mapped = (
            bias2
            + moved[1]
            + jnp.where(column > 0, moved[0], 0.0)
            + jnp.where(column < SIDE - 1, moved[2], 0.0)
        )
        scored = jnp.maximum(mapped, 0.0) * head_ref[:, first:first + LANES].T
        running = running + jnp.sum(scored.reshape(LANES // 8, 8, width), axis=0)
    out_ref[...] = jnp.broadcast_to(jnp.sum(running), out_ref.shape)


def score(types, pose_total, own, near, far, head_own, head_far, folded, bias1, weight2, bias2, copies):
    plane_cells = own.shape[1]
    depth, mid = folded.shape[1:]
    width = weight2.shape[2]
    padded = round_up(plane_cells // 2 + 2 * SIDE, TILE)
    return pl.pallas_call(
        functools.partial(score_kernel, pose_total, types),
        out_shape=pltpu.VMEM((copies, LANES), f32),
        scratch_shapes=[
            pltpu.VMEM((8, plane_cells + 3 * LANES), jnp.int32),
            pltpu.VMEM((5, padded, depth), bf16),
            pltpu.VMEM((3, padded, mid), bf16),
            pltpu.VMEM((9, padded + 16, width), f32),
            pltpu.VMEM((width, plane_cells // 2), f32),
        ],
        compiler_params=params(40),
        name="score",
    )(
        in_vmem(own),
        in_vmem(near),
        in_vmem(far),
        in_vmem(head_own),
        in_vmem(head_far),
        in_vmem(folded),
        in_vmem(bias1),
        in_vmem(weight2),
        in_vmem(bias2),
    )


def final_kernel(pose_total, chan_count, parts_ref, plane_ref, scores_ref):
    parts = parts_ref[:, 0, :]
    pose = lax.broadcasted_iota(jnp.int32, parts.shape, 0) // chan_count
    first = lax.broadcasted_iota(jnp.int32, parts.shape, 1) == 0
    plane_ref[0] = jnp.sum(jnp.where(first & (pose == lax.axis_index("pose")), parts, 0.0))
    for p in range(pose_total):
        scores_ref[p] = jnp.sum(jnp.where(first & (lax.rem(pose, pose_total) == p), parts, 0.0))


def final_sums(parts, pose_total, chan_count):
    smem = pl.BlockSpec(memory_space=pltpu.SMEM)
    return pl.pallas_call(
        functools.partial(final_kernel, pose_total, chan_count),
        out_shape=(
            jax.ShapeDtypeStruct((1,), f32),
            jax.ShapeDtypeStruct((pose_total,), f32),
        ),
        out_specs=(smem, smem),
        compiler_params=params(1),
        name="final_sums",
    )(in_vmem(parts))


def on_device(
    atom_type,
    occupancy,
    atom_embed,
    conv1_weight,
    conv1_bias,
    conv2_weight,
    conv2_bias,
    head_weight,
):
    chan_count = lax.axis_size("chan")
    pose_count = lax.axis_size("pose")
    pose_total = pose_count // XPLANES
    swap = [(0, 1), (1, 0)]

    def fetch(steps):
        by = steps * pose_total
        pairs = []
        for i in range(pose_count):
            up = 2 * (i + by) + 1 if i + by < pose_count else 2 * i
            down = 2 * (i - by) if i >= by else 2 * i + 1
            pairs += [(2 * i, down), (2 * i + 1, up)]
        return lax.ppermute(code, ("pose", "chan"), pairs)

    types = atom_embed.shape[0]
    code, pair = encode(atom_type, occupancy, atom_embed)
    second, first, folded = lax.optimization_barrier(
        (fetch(2), fetch(1), fold_embedding(types, pair, conv1_weight))
    )
    near = jnp.concatenate([first, second], axis=1)
    far = lax.ppermute(near, "chan", swap)
    head_far = lax.ppermute(head_weight, "chan", swap)
    part = score(
        types,
        pose_total,
        code,
        near,
        far,
        head_weight,
        head_far,
        folded,
        conv1_bias[None, :],
        conv2_weight,
        conv2_bias[None, :],
        pose_count * chan_count,
    )
    parts = lax.all_to_all(part[:, None, :], ("pose", "chan"), 0, 0, tiled=True)
    return final_sums(parts, pose_total, chan_count)


def solution(mesh):
    return jax.shard_map(
        on_device,
        mesh=mesh,
        in_specs=(P("pose", None), P("pose", None), P(), P(), P(), P(), P(), P("chan", None)),
        out_specs=(P("pose"), P()),
        check_vma=False,
    )
```

```python
import functools

import jax
import jax.numpy as jnp
from jax import lax
from jax.experimental import pallas as pl
from jax.experimental.pallas import tpu as pltpu
from jax.sharding import PartitionSpec as P

SIDE = 48
XPLANES = 16
LANES = 128
TILE = 256
PARTS = 3
TAPS = [(shift_y, shift_z) for shift_y in (-1, 0, 1) for shift_z in (-1, 0, 1)]

bf16 = jnp.bfloat16
f32 = jnp.float32


def in_vmem(array):
    return pltpu.with_memory_space_constraint(array, pltpu.VMEM)


def in_hbm(array):
    return pltpu.with_memory_space_constraint(array, pltpu.HBM)


def round_up(value, step):
    return -(-value // step) * step


def params(megabytes):
    return pltpu.CompilerParams(vmem_limit_bytes=megabytes << 20)


def encode_kernel(type_hbm, count_hbm, embed_hbm, code_ref, pair_ref, type_ref, count_ref, embed_ref, sems):
    types = embed_ref.shape[0]
    half = pair_ref.shape[0] // 2
    copies = [
        pltpu.make_async_copy(source, target, sems.at[n])
        for n, (source, target) in enumerate(
            ((type_hbm, type_ref), (count_hbm, count_ref), (embed_hbm, embed_ref))
        )
    ]
    for copy in copies:
        copy.start()
    pair_ref[...] = jnp.zeros_like(pair_ref)
    for copy in copies:
        copy.wait()
    code_ref[...] = type_ref[...] * 4 + count_ref[...]
    embed = embed_ref[...].astype(f32)
    pair_ref[:types, :] = embed
    pair_ref[half:half + types, :] = (3.0 * embed).astype(bf16).astype(f32)


def encode(atom_type, occupancy, atom_embed):
    types, width = atom_embed.shape
    return pl.pallas_call(
        encode_kernel,
        out_shape=(
            pltpu.VMEM(atom_type.shape, jnp.int32),
            pltpu.VMEM((2 * round_up(types, 16), width), f32),
        ),
        in_specs=[pl.BlockSpec(memory_space=pl.ANY)] * 3,
        scratch_shapes=[
            pltpu.VMEM(atom_type.shape, jnp.int32),
            pltpu.VMEM(atom_type.shape, jnp.int32),
            pltpu.VMEM(atom_embed.shape, bf16),
            pltpu.SemaphoreType.DMA((3,)),
        ],
        compiler_params=params(1),
        cost_estimate=pl.CostEstimate(flops=4 * 10**9, bytes_accessed=8 << 20, transcendentals=0),
        name="encode",
    )(in_hbm(atom_type), in_hbm(occupancy), in_hbm(atom_embed))


def fold_kernel(types, pair_ref, weight_ref, folded_ref, rows_ref):
    half = pair_ref.shape[0] // 2
    rest = round_up(9 * types, LANES)
    pair = pair_ref[...].astype(bf16)
    rows_ref[...] = jnp.zeros_like(rows_ref)
    for dx in range(3):
        for tap in range(9):
            both = jnp.dot(pair, weight_ref[dx * 9 + tap], preferred_element_type=f32)
            once, thrice = both[:types, :], both[half:half + types, :]
            rounded = once.astype(bf16).astype(f32)
            first = rest + 2 * types * tap
            rows_ref[dx, types * tap:types * (tap + 1), :] = rounded
            rows_ref[dx, first:first + types, :] = once - rounded
            rows_ref[dx, first + types:first + 2 * types, :] = thrice - 3.0 * rounded
        folded_ref[dx] = rows_ref[dx].astype(bf16)


def fold_embedding(types, pair, conv1_weight):
    mid = conv1_weight.shape[2]
    depth = round_up(9 * types, LANES) + round_up(18 * types, LANES)
    return pl.pallas_call(
        functools.partial(fold_kernel, types),
        out_shape=pltpu.VMEM((3, depth, mid), bf16),
        scratch_shapes=[pltpu.VMEM((3, depth, mid), f32)],
        compiler_params=params(12),
        name="fold_embedding",
    )(in_vmem(pair), in_vmem(conv1_weight))


def one_hot(rows, x, types, start):
    width = TILE
    depth = round_up(types * len(rows), LANES)
    sub = lax.broadcasted_iota(jnp.int32, (8, 1), 0)

    def spread(row):
        return jnp.broadcast_to(row[x:x + 1, start:start + width], (8, width))

    groups = []
    for first in range(0, depth, 8):
        low, high = first // types, (first + 7) // types
        if low >= len(rows):
            groups.append(jnp.zeros((8, width), f32))
            continue
        kind, count = spread(rows[low][0]), spread(rows[low][1])
        number = sub + (first - types * low)
        if high != low:
            own = sub < types * high - first
            number = jnp.where(own, number, number - types)
            if high < len(rows):
                kind = jnp.where(own, kind, spread(rows[high][0]))
                count = jnp.where(own, count, spread(rows[high][1]))
            else:
                count = jnp.where(own, count, 0.0)
        groups.append(jnp.where(kind == number, count, 0.0))
    return jnp.concatenate(groups, axis=0)


def tap_rows(planes_ref, rows, chan, padded, types):
    plane_cells = rows[0].shape[1]
    half_cells = plane_cells // 2
    planes_ref[...] = jnp.zeros_like(planes_ref)
    for x, row in enumerate(rows):
        planes_ref[x:x + 1, LANES:LANES + plane_cells] = row
    start = pl.multiple_of(chan * half_cells, LANES)
    cells = planes_ref[:, pl.ds(start, half_cells + 3 * LANES)]
    column = lax.rem(lax.broadcasted_iota(jnp.int32, (8, padded), 1), SIDE)
    plain, split = [], []
    for shift_y, shift_z in TAPS:
        first = LANES - SIDE + SIDE * shift_y + shift_z
        moved = cells[:, first:first + padded]
        inside = (column + shift_z >= 0) & (column + shift_z < SIDE)
        moved = jnp.where(inside, moved, 0)
        kind = lax.shift_right_logical(moved, 2)
        count = moved & 3
        plain.append((kind, count.astype(f32)))
        split.append(
            (
                jnp.where(count == 3, kind + types, kind),
                jnp.where(count == 3, 1, count).astype(f32),
            )
        )
    return plain, split


def both_hot(plain, split, x, types, first):
    return jnp.concatenate(
        [one_hot(plain, x, types, first), one_hot(split, x, 2 * types, first)], axis=0
    ).astype(bf16).T


def hidden_rows(operands, bias1, folded_ref, first, size, half_cells, chan, plane_ok):
    total = bias1
    for dx in range(3):
        total = total + jnp.dot(
            operands[dx](first, size), folded_ref[dx], preferred_element_type=f32
        )
    index = first + lax.broadcasted_iota(jnp.int32, (size, 1), 0)
    lowest = jnp.where(plane_ok, jnp.where(chan == 0, SIDE, 0), half_cells + 2 * SIDE)
    highest = jnp.where(chan == 0, half_cells + 2 * SIDE, half_cells + SIDE)
    inside = (index >= lowest) & (index < highest)
    return jnp.where(inside, jnp.maximum(total, 0.0), 0.0).astype(bf16)


def reader(ref, x):
    return lambda first, size: ref[x, first:first + size, :]


def score_kernel(
    pose_total,
    types,
    own_ref,
    near_ref,
    far_ref,
    head_own_ref,
    head_far_ref,
    folded_ref,
    bias1_ref,
    weight2_ref,
    bias2_ref,
    out_ref,
    planes_ref,
    hot_ref,
    hidden_ref,
    sums_ref,
    head_ref,
):
    chan = lax.axis_index("chan")
    block = lax.axis_index("pose") // pose_total
    plane_cells = own_ref.shape[1]
    half_cells = plane_cells // 2
    padded = hot_ref.shape[1]
    used = half_cells + 2 * SIDE
    share = head_own_ref.shape[0]
    head_cells = pl.ds(pl.multiple_of(chan * half_cells, LANES), half_cells)
    head_ref[pl.ds(pl.multiple_of(chan * share, share), share), :] = head_own_ref[:, head_cells]
    head_ref[pl.ds(pl.multiple_of((1 - chan) * share, share), share), :] = head_far_ref[
        :, head_cells
    ]
    near, far = near_ref[...], far_ref[...]
    sides = []
    for step in (1, 2):
        cells = slice((step - 1) * plane_cells, step * plane_cells)
        end = (block < step) | (block >= XPLANES - step)
        above = (chan == lax.rem(block // step, 2)) != end
        sides.append(
            (
                jnp.where(block >= step, jnp.where(above, far[:, cells], near[:, cells]), 0),
                jnp.where(
                    block < XPLANES - step, jnp.where(above, near[:, cells], far[:, cells]), 0
                ),
            )
        )
    rows = [sides[1][0], sides[0][0], own_ref[...], sides[0][1], sides[1][1]]
    plain, split = tap_rows(planes_ref, rows, chan, padded, types)
    bias1 = bias1_ref[...]
    operands = [reader(hot_ref, x) for x in range(5)]
    plane_ok = [block >= 1, True, block <= XPLANES - 2]
    for first in range(0, padded, TILE):
        size = min(TILE, used - first)
        for x in range(5):
            hot_ref[x, first:first + TILE, :] = both_hot(plain, split, x, types, first)
            if x >= 2:
                h = x - 2
                hidden_ref[h, first:first + size, :] = hidden_rows(
                    operands[h:], bias1, folded_ref, first, size, half_cells, chan, plane_ok[h]
                )

    width = weight2_ref.shape[2]
    hidden = [reader(hidden_ref, h) for h in range(3)]

    def taps(first, size, *numbers):
        total = None
        for h in range(3):
            weights = [weight2_ref[h * 9 + tap] for tap in numbers]
            part = jnp.dot(
                hidden[h](first, size),
                jnp.concatenate(weights, axis=1),
                preferred_element_type=f32,
            )
            total = part if total is None else total + part
        return [total[:, n * width:(n + 1) * width] for n in range(len(numbers))]

    ends = [(0, half_cells), (0, half_cells + SIDE), (SIDE, half_cells + SIDE), (2 * SIDE, used), (2 * SIDE, used)]
    for pair, (begin, end) in enumerate(ends):
        size = (end - begin) // PARTS
        numbers = [2 * pair, 2 * pair + 1][: 2 if pair < 4 else 1]
        for first in range(begin, end, size):
            for number, value in zip(numbers, taps(first, size, *numbers)):
                sums_ref[number, 8 + first:8 + first + size, :] = value
    bias2 = bias2_ref[...]
    running = jnp.zeros((8, width), f32)
    for first in range(0, half_cells, LANES):
        moved = []
        for shift_z in range(3):
            offset = 8 + first + shift_z - 1
            moved.append(
                sums_ref[shift_z, offset:offset + LANES, :]
                + sums_ref[3 + shift_z, offset + SIDE:offset + SIDE + LANES, :]
                + sums_ref[6 + shift_z, offset + 2 * SIDE:offset + 2 * SIDE + LANES, :]
            )
        column = lax.rem(first + lax.broadcasted_iota(jnp.int32, (LANES, 1), 0), SIDE)
        mapped = (
            bias2
            + moved[1]
            + jnp.where(column > 0, moved[0], 0.0)
            + jnp.where(column < SIDE - 1, moved[2], 0.0)
        )
        scored = jnp.maximum(mapped, 0.0) * head_ref[:, first:first + LANES].T
        running = running + jnp.sum(scored.reshape(LANES // 8, 8, width), axis=0)
    out_ref[...] = jnp.broadcast_to(jnp.sum(running), out_ref.shape)


def score(types, pose_total, own, near, far, head_own, head_far, folded, bias1, weight2, bias2, copies):
    plane_cells = own.shape[1]
    depth, mid = folded.shape[1:]
    width = weight2.shape[2]
    padded = round_up(plane_cells // 2 + 2 * SIDE, TILE)
    return pl.pallas_call(
        functools.partial(score_kernel, pose_total, types),
        out_shape=pltpu.VMEM((copies, LANES), f32),
        scratch_shapes=[
            pltpu.VMEM((8, plane_cells + 3 * LANES), jnp.int32),
            pltpu.VMEM((5, padded, depth), bf16),
            pltpu.VMEM((3, padded, mid), bf16),
            pltpu.VMEM((9, padded + 16, width), f32),
            pltpu.VMEM((width, plane_cells // 2), f32),
        ],
        compiler_params=params(40),
        name="score",
    )(
        in_vmem(own),
        in_vmem(near),
        in_vmem(far),
        in_vmem(head_own),
        in_vmem(head_far),
        in_vmem(folded),
        in_vmem(bias1),
        in_vmem(weight2),
        in_vmem(bias2),
    )


def final_kernel(pose_total, chan_count, parts_ref, plane_ref, scores_ref):
    parts = parts_ref[:, 0, :]
    pose = lax.broadcasted_iota(jnp.int32, parts.shape, 0) // chan_count
    first = lax.broadcasted_iota(jnp.int32, parts.shape, 1) == 0
    plane_ref[0] = jnp.sum(jnp.where(first & (pose == lax.axis_index("pose")), parts, 0.0))
    for p in range(pose_total):
        scores_ref[p] = jnp.sum(jnp.where(first & (lax.rem(pose, pose_total) == p), parts, 0.0))


def final_sums(parts, pose_total, chan_count):
    smem = pl.BlockSpec(memory_space=pltpu.SMEM)
    return pl.pallas_call(
        functools.partial(final_kernel, pose_total, chan_count),
        out_shape=(
            jax.ShapeDtypeStruct((1,), f32),
            jax.ShapeDtypeStruct((pose_total,), f32),
        ),
        out_specs=(smem, smem),
        compiler_params=params(1),
        name="final_sums",
    )(in_vmem(parts))


def on_device(
    atom_type,
    occupancy,
    atom_embed,
    conv1_weight,
    conv1_bias,
    conv2_weight,
    conv2_bias,
    head_weight,
):
    chan_count = lax.axis_size("chan")
    pose_count = lax.axis_size("pose")
    pose_total = pose_count // XPLANES
    swap = [(0, 1), (1, 0)]

    def fetch(step):
        pairs = []
        for i in range(pose_count):
            above = i // pose_total // step % 2
            sources = {}
            for core, other in ((above, i + step * pose_total), (1 - above, i - step * pose_total)):
                if 0 <= other < pose_count:
                    sources[core] = 2 * other + core
            for core in (0, 1):
                if core not in sources:
                    sources[core], sources[1 - core] = sources[1 - core], 2 * i + core
            pairs += [(sources[core], 2 * i + core) for core in (0, 1)]
        return lax.ppermute(code, ("pose", "chan"), pairs)

    types = atom_embed.shape[0]
    code, pair = encode(atom_type, occupancy, atom_embed)
    second, first, folded = lax.optimization_barrier(
        (fetch(2), fetch(1), fold_embedding(types, pair, conv1_weight))
    )
    near = jnp.concatenate([first, second], axis=1)
    far = lax.ppermute(near, "chan", swap)
    head_far = lax.ppermute(head_weight, "chan", swap)
    part = score(
        types,
        pose_total,
        code,
        near,
        far,
        head_weight,
        head_far,
        folded,
        conv1_bias[None, :],
        conv2_weight,
        conv2_bias[None, :],
        pose_count * chan_count,
    )
    parts = lax.all_to_all(part[:, None, :], ("pose", "chan"), 0, 0, tiled=True)
    return final_sums(parts, pose_total, chan_count)


def solution(mesh):
    return jax.shard_map(
        on_device,
        mesh=mesh,
        in_specs=(P("pose", None), P("pose", None), P(), P(), P(), P(), P(), P("chan", None)),
        out_specs=(P("pose"), P()),
        check_vma=False,
    )
```

```python
import functools

import jax
import jax.numpy as jnp
from jax import lax
from jax.experimental import pallas as pl
from jax.experimental.pallas import tpu as pltpu
from jax.sharding import PartitionSpec as P

SIDE = 48
XPLANES = 16
LANES = 128
TILE = 640
STEP = 1152
TAPS = [(shift_y, shift_z) for shift_y in (-1, 0, 1) for shift_z in (-1, 0, 1)]

bf16 = jnp.bfloat16
f32 = jnp.float32


def in_vmem(array):
    return pltpu.with_memory_space_constraint(array, pltpu.VMEM)


def in_hbm(array):
    return pltpu.with_memory_space_constraint(array, pltpu.HBM)


def round_up(value, step):
    return -(-value // step) * step


def params(megabytes):
    return pltpu.CompilerParams(vmem_limit_bytes=megabytes << 20)


def encode_kernel(type_hbm, count_hbm, embed_hbm, code_ref, pair_ref, type_ref, count_ref, embed_ref, sems):
    types = embed_ref.shape[0]
    half = pair_ref.shape[0] // 2
    copies = [
        pltpu.make_async_copy(source, target, sems.at[n])
        for n, (source, target) in enumerate(
            ((type_hbm, type_ref), (count_hbm, count_ref), (embed_hbm, embed_ref))
        )
    ]
    for copy in copies:
        copy.start()
    pair_ref[...] = jnp.zeros_like(pair_ref)
    for copy in copies:
        copy.wait()
    code_ref[...] = type_ref[...] * 4 + count_ref[...]
    embed = embed_ref[...].astype(f32)
    pair_ref[:types, :] = embed
    pair_ref[half:half + types, :] = (3.0 * embed).astype(bf16).astype(f32)


def encode(atom_type, occupancy, atom_embed):
    types, width = atom_embed.shape
    return pl.pallas_call(
        encode_kernel,
        out_shape=(
            pltpu.VMEM(atom_type.shape, jnp.int32),
            pltpu.VMEM((2 * round_up(types, 16), width), f32),
        ),
        in_specs=[pl.BlockSpec(memory_space=pl.ANY)] * 3,
        scratch_shapes=[
            pltpu.VMEM(atom_type.shape, jnp.int32),
            pltpu.VMEM(atom_type.shape, jnp.int32),
            pltpu.VMEM(atom_embed.shape, bf16),
            pltpu.SemaphoreType.DMA((3,)),
        ],
        compiler_params=params(1),
        cost_estimate=pl.CostEstimate(flops=4 * 10**9, bytes_accessed=8 << 20, transcendentals=0),
        name="encode",
    )(in_hbm(atom_type), in_hbm(occupancy), in_hbm(atom_embed))


def fold_kernel(types, pair_ref, weight_ref, folded_ref, rows_ref):
    half = pair_ref.shape[0] // 2
    rest = round_up(9 * types, LANES)
    pair = pair_ref[...].astype(bf16)
    rows_ref[...] = jnp.zeros_like(rows_ref)
    for dx in range(3):
        for tap in range(9):
            both = jnp.dot(pair, weight_ref[dx * 9 + tap], preferred_element_type=f32)
            once, thrice = both[:types, :], both[half:half + types, :]
            rounded = once.astype(bf16).astype(f32)
            first = rest + 2 * types * tap
            rows_ref[dx, types * tap:types * (tap + 1), :] = rounded
            rows_ref[dx, first:first + types, :] = once - rounded
            rows_ref[dx, first + types:first + 2 * types, :] = thrice - 3.0 * rounded
        folded_ref[dx] = rows_ref[dx].astype(bf16)


def fold_embedding(types, pair, conv1_weight):
    mid = conv1_weight.shape[2]
    depth = round_up(9 * types, LANES) + round_up(18 * types, LANES)
    return pl.pallas_call(
        functools.partial(fold_kernel, types),
        out_shape=pltpu.VMEM((3, depth, mid), bf16),
        scratch_shapes=[pltpu.VMEM((3, depth, mid), f32)],
        compiler_params=params(12),
        name="fold_embedding",
    )(in_vmem(pair), in_vmem(conv1_weight))


def one_hot(rows, x, types, start):
    shape = (16, TILE)
    sub = lax.broadcasted_iota(jnp.int32, shape, 0).astype(f32).astype(bf16)
    empty = jnp.zeros(shape, bf16)

    def spread(row):
        return jnp.broadcast_to(row[x:x + 1, start:start + TILE], shape).astype(bf16)

    kinds = [spread(kind) for kind, _ in rows]
    counts = [spread(count) for _, count in rows]
    groups = []
    for first in range(0, round_up(types * len(rows), LANES), 16):
        low, high = first // types, (first + 15) // types
        if low >= len(rows):
            groups.append(empty)
            continue
        group = jnp.where(kinds[low] == sub + bf16(first - types * low), counts[low], empty)
        if high != low and high < len(rows):
            group = jnp.where(
                kinds[high] == sub + bf16(first - types * high), counts[high], group
            )
        groups.append(group)
    return jnp.concatenate(groups, axis=0)


def tap_rows(planes_ref, rows, chan, padded, types):
    plane_cells = rows[0].shape[1]
    half_cells = plane_cells // 2
    planes_ref[...] = jnp.zeros_like(planes_ref)
    for x, row in enumerate(rows):
        planes_ref[x:x + 1, LANES:LANES + plane_cells] = row
    start = pl.multiple_of(chan * half_cells, LANES)
    cells = planes_ref[:, pl.ds(start, half_cells + 3 * LANES)]
    column = lax.rem(lax.broadcasted_iota(jnp.int32, (8, padded), 1), SIDE)
    plain, split = [], []
    for shift_y, shift_z in TAPS:
        first = LANES - SIDE + SIDE * shift_y + shift_z
        moved = cells[:, first:first + padded]
        inside = (column + shift_z >= 0) & (column + shift_z < SIDE)
        moved = jnp.where(inside, moved, 0)
        kind = lax.shift_right_logical(moved, 2)
        count = moved & 3
        plain.append((kind.astype(f32), count.astype(f32)))
        split.append(
            (
                jnp.where(count == 3, kind + types, kind).astype(f32),
                jnp.where(count == 3, 1, count).astype(f32),
            )
        )
    return plain, split


def both_hot(plain, split, x, types, first):
    return jnp.concatenate(
        [one_hot(plain, x, types, first), one_hot(split, x, 2 * types, first)], axis=0
    ).T


def hidden_rows(operands, bias1, folded_ref, first, size, half_cells, chan, plane_ok):
    total = bias1
    for dx in range(3):
        total = total + jnp.dot(
            operands[dx](first, size), folded_ref[dx], preferred_element_type=f32
        )
    index = first + lax.broadcasted_iota(jnp.int32, (size, 1), 0)
    lowest = jnp.where(plane_ok, jnp.where(chan == 0, SIDE, 0), half_cells + 2 * SIDE)
    highest = jnp.where(chan == 0, half_cells + 2 * SIDE, half_cells + SIDE)
    inside = (index >= lowest) & (index < highest)
    return jnp.where(inside, jnp.maximum(total, 0.0), 0.0).astype(bf16)


def reader(ref, x):
    return lambda first, size: ref[x, first:first + size, :]


def score_kernel(
    pose_total,
    types,
    own_ref,
    near_ref,
    far_ref,
    head_own_ref,
    head_far_ref,
    folded_ref,
    bias1_ref,
    weight2_ref,
    bias2_ref,
    out_ref,
    planes_ref,
    hot_ref,
    hidden_ref,
    sums_ref,
    head_ref,
):
    chan = lax.axis_index("chan")
    block = lax.axis_index("pose") // pose_total
    plane_cells = own_ref.shape[1]
    half_cells = plane_cells // 2
    padded = hot_ref.shape[1]
    used = half_cells + 2 * SIDE
    share = head_own_ref.shape[0]
    head_cells = pl.ds(pl.multiple_of(chan * half_cells, LANES), half_cells)
    head_ref[pl.ds(pl.multiple_of(chan * share, share), share), :] = head_own_ref[:, head_cells]
    head_ref[pl.ds(pl.multiple_of((1 - chan) * share, share), share), :] = head_far_ref[
        :, head_cells
    ]
    near, far = near_ref[...], far_ref[...]
    sides = []
    for step in (1, 2):
        cells = slice((step - 1) * plane_cells, step * plane_cells)
        end = (block < step) | (block >= XPLANES - step)
        above = (chan == lax.rem(block // step, 2)) != end
        sides.append(
            (
                jnp.where(block >= step, jnp.where(above, far[:, cells], near[:, cells]), 0),
                jnp.where(
                    block < XPLANES - step, jnp.where(above, near[:, cells], far[:, cells]), 0
                ),
            )
        )
    rows = [sides[1][0], sides[0][0], own_ref[...], sides[0][1], sides[1][1]]
    plain, split = tap_rows(planes_ref, rows, chan, padded, types)
    bias1 = bias1_ref[...]
    operands = [reader(hot_ref, x) for x in range(5)]
    plane_ok = [block >= 1, True, block <= XPLANES - 2]
    for first in range(0, padded, TILE):
        size = min(TILE, used - first)
        for x in range(5):
            hot_ref[x, first:first + TILE, :] = both_hot(plain, split, x, types, first)
            if x >= 2:
                h = x - 2
                hidden_ref[h, first:first + size, :] = hidden_rows(
                    operands[h:], bias1, folded_ref, first, size, half_cells, chan, plane_ok[h]
                )

    width = weight2_ref.shape[2]
    hidden = [reader(hidden_ref, h) for h in range(3)]

    def taps(first, size, *numbers):
        total = None
        for h in range(3):
            weights = [weight2_ref[h * 9 + tap] for tap in numbers]
            part = jnp.dot(
                hidden[h](first, size),
                jnp.concatenate(weights, axis=1),
                preferred_element_type=f32,
            )
            total = part if total is None else total + part
        return [total[:, n * width:(n + 1) * width] for n in range(len(numbers))]

    bias2 = bias2_ref[...]
    step = STEP
    column = lax.rem(lax.broadcasted_iota(jnp.int32, (step, 1), 0), SIDE)
    running = jnp.zeros((8, width), f32)
    for first in range(0, half_cells, step):
        tap0, tap1 = taps(first, step, 0, 1)
        tap2, tap3 = taps(first, step + SIDE, 2, 3)
        tap4, tap5 = taps(first + SIDE, step, 4, 5)
        tap6, tap7 = taps(first + 2 * SIDE, step, 6, 7)
        (tap8,) = taps(first + 2 * SIDE, step, 8)
        sums_ref[0, 8 + first:8 + first + step, :] = tap0 + tap3[SIDE:] + tap6
        middle = bias2 + tap1 + tap4 + tap7
        sums_ref[1, 8 + first:8 + first + step, :] = tap2[:step] + tap5 + tap8
        mapped = (
            middle
            + jnp.where(column > 0, sums_ref[0, 7 + first:7 + first + step, :], 0.0)
            + jnp.where(column < SIDE - 1, sums_ref[1, 9 + first:9 + first + step, :], 0.0)
        )
        scored = jnp.maximum(mapped, 0.0) * head_ref[:, first:first + step].T
        running = running + jnp.sum(scored.reshape(step // 8, 8, width), axis=0)
    out_ref[...] = jnp.broadcast_to(jnp.sum(running), out_ref.shape)


def score(types, pose_total, own, near, far, head_own, head_far, folded, bias1, weight2, bias2, copies):
    plane_cells = own.shape[1]
    depth, mid = folded.shape[1:]
    width = weight2.shape[2]
    padded = round_up(plane_cells // 2 + 2 * SIDE, TILE)
    return pl.pallas_call(
        functools.partial(score_kernel, pose_total, types),
        out_shape=pltpu.VMEM((copies, LANES), f32),
        scratch_shapes=[
            pltpu.VMEM((8, plane_cells + 3 * LANES), jnp.int32),
            pltpu.VMEM((5, padded, depth), bf16),
            pltpu.VMEM((3, padded, mid), bf16),
            pltpu.VMEM((2, plane_cells // 2 + 16, width), f32),
            pltpu.VMEM((width, plane_cells // 2), f32),
        ],
        compiler_params=params(40),
        name="score",
    )(
        in_vmem(own),
        in_vmem(near),
        in_vmem(far),
        in_vmem(head_own),
        in_vmem(head_far),
        in_vmem(folded),
        in_vmem(bias1),
        in_vmem(weight2),
        in_vmem(bias2),
    )


def final_kernel(pose_total, chan_count, parts_ref, plane_ref, scores_ref):
    parts = parts_ref[:, 0, :]
    pose = lax.broadcasted_iota(jnp.int32, parts.shape, 0) // chan_count
    first = lax.broadcasted_iota(jnp.int32, parts.shape, 1) == 0
    plane_ref[0] = jnp.sum(jnp.where(first & (pose == lax.axis_index("pose")), parts, 0.0))
    for p in range(pose_total):
        scores_ref[p] = jnp.sum(jnp.where(first & (lax.rem(pose, pose_total) == p), parts, 0.0))


def final_sums(parts, pose_total, chan_count):
    smem = pl.BlockSpec(memory_space=pltpu.SMEM)
    return pl.pallas_call(
        functools.partial(final_kernel, pose_total, chan_count),
        out_shape=(
            jax.ShapeDtypeStruct((1,), f32),
            jax.ShapeDtypeStruct((pose_total,), f32),
        ),
        out_specs=(smem, smem),
        compiler_params=params(1),
        name="final_sums",
    )(in_vmem(parts))


def on_device(
    atom_type,
    occupancy,
    atom_embed,
    conv1_weight,
    conv1_bias,
    conv2_weight,
    conv2_bias,
    head_weight,
):
    chan_count = lax.axis_size("chan")
    pose_count = lax.axis_size("pose")
    pose_total = pose_count // XPLANES
    swap = [(0, 1), (1, 0)]

    def fetch(step):
        pairs = []
        for i in range(pose_count):
            above = i // pose_total // step % 2
            sources = {}
            for core, other in ((above, i + step * pose_total), (1 - above, i - step * pose_total)):
                if 0 <= other < pose_count:
                    sources[core] = 2 * other + core
            for core in (0, 1):
                if core not in sources:
                    sources[core], sources[1 - core] = sources[1 - core], 2 * i + core
            pairs += [(sources[core], 2 * i + core) for core in (0, 1)]
        return lax.ppermute(code, ("pose", "chan"), pairs)

    types = atom_embed.shape[0]
    code, pair = encode(atom_type, occupancy, atom_embed)
    second, first, folded = lax.optimization_barrier(
        (fetch(2), fetch(1), fold_embedding(types, pair, conv1_weight))
    )
    near = jnp.concatenate([first, second], axis=1)
    far = lax.ppermute(near, "chan", swap)
    head_far = lax.ppermute(head_weight, "chan", swap)
    part = score(
        types,
        pose_total,
        code,
        near,
        far,
        head_weight,
        head_far,
        folded,
        conv1_bias[None, :],
        conv2_weight,
        conv2_bias[None, :],
        pose_count * chan_count,
    )
    parts = lax.all_to_all(part[:, None, :], ("pose", "chan"), 0, 0, tiled=True)
    return final_sums(parts, pose_total, chan_count)


def solution(mesh):
    return jax.shard_map(
        on_device,
        mesh=mesh,
        in_specs=(P("pose", None), P("pose", None), P(), P(), P(), P(), P(), P("chan", None)),
        out_specs=(P("pose"), P()),
        check_vma=False,
    )
```

```python
import functools

import jax
import jax.numpy as jnp
from jax import lax
from jax.experimental import pallas as pl
from jax.experimental.pallas import tpu as pltpu
from jax.sharding import PartitionSpec as P

SIDE = 48
XPLANES = 16
LANES = 128
TILE = 640
STEP = 1152
TAPS = [(shift_y, shift_z) for shift_y in (-1, 0, 1) for shift_z in (-1, 0, 1)]

bf16 = jnp.bfloat16
f32 = jnp.float32


def in_vmem(array):
    return pltpu.with_memory_space_constraint(array, pltpu.VMEM)


def in_hbm(array):
    return pltpu.with_memory_space_constraint(array, pltpu.HBM)


def round_up(value, step):
    return -(-value // step) * step


def params(megabytes):
    return pltpu.CompilerParams(vmem_limit_bytes=megabytes << 20)


def encode_kernel(type_hbm, count_hbm, code_ref, type_ref, count_ref, sems):
    copies = [
        pltpu.make_async_copy(source, target, sems.at[n])
        for n, (source, target) in enumerate(((type_hbm, type_ref), (count_hbm, count_ref)))
    ]
    for copy in copies:
        copy.start()
    for copy in copies:
        copy.wait()
    code_ref[...] = type_ref[...] * 4 + count_ref[...]


def encode(atom_type, occupancy):
    return pl.pallas_call(
        encode_kernel,
        out_shape=pltpu.VMEM(atom_type.shape, jnp.int32),
        in_specs=[pl.BlockSpec(memory_space=pl.ANY)] * 2,
        scratch_shapes=[
            pltpu.VMEM(atom_type.shape, jnp.int32),
            pltpu.VMEM(atom_type.shape, jnp.int32),
            pltpu.SemaphoreType.DMA((2,)),
        ],
        compiler_params=params(1),
        cost_estimate=pl.CostEstimate(flops=4 * 10**9, bytes_accessed=8 << 20, transcendentals=0),
        name="encode",
    )(in_hbm(atom_type), in_hbm(occupancy))


def fold_kernel(embed_ref, weight_ref, folded_ref, pair_ref, rows_ref):
    types = embed_ref.shape[0]
    half = pair_ref.shape[0] // 2
    embed = embed_ref[...].astype(f32)
    pair_ref[...] = jnp.zeros_like(pair_ref)
    pair_ref[:types, :] = embed
    pair_ref[half:half + types, :] = (3.0 * embed).astype(bf16).astype(f32)
    rest = round_up(9 * types, LANES)
    pair = pair_ref[...].astype(bf16)
    rows_ref[...] = jnp.zeros_like(rows_ref)
    for dx in range(3):
        for tap in range(9):
            both = jnp.dot(pair, weight_ref[dx * 9 + tap], preferred_element_type=f32)
            once, thrice = both[:types, :], both[half:half + types, :]
            rounded = once.astype(bf16).astype(f32)
            first = rest + 2 * types * tap
            rows_ref[dx, types * tap:types * (tap + 1), :] = rounded
            rows_ref[dx, first:first + types, :] = once - rounded
            rows_ref[dx, first + types:first + 2 * types, :] = thrice - 3.0 * rounded
        folded_ref[dx] = rows_ref[dx].astype(bf16)


def fold_embedding(atom_embed, conv1_weight):
    types, width = atom_embed.shape
    mid = conv1_weight.shape[2]
    depth = round_up(9 * types, LANES) + round_up(18 * types, LANES)
    return pl.pallas_call(
        fold_kernel,
        out_shape=pltpu.VMEM((3, depth, mid), bf16),
        scratch_shapes=[
            pltpu.VMEM((2 * round_up(types, 16), width), f32),
            pltpu.VMEM((3, depth, mid), f32),
        ],
        compiler_params=params(12),
        name="fold_embedding",
    )(in_vmem(atom_embed), in_vmem(conv1_weight))


def one_hot(rows, x, types, start):
    shape = (16, TILE)
    sub = lax.broadcasted_iota(jnp.int32, shape, 0).astype(f32).astype(bf16)
    empty = jnp.zeros(shape, bf16)

    def spread(row):
        return jnp.broadcast_to(row[x:x + 1, start:start + TILE], shape).astype(bf16)

    kinds = [spread(kind) for kind, _ in rows]
    counts = [spread(count) for _, count in rows]
    groups = []
    for first in range(0, round_up(types * len(rows), LANES), 16):
        low, high = first // types, (first + 15) // types
        if low >= len(rows):
            groups.append(empty)
            continue
        group = jnp.where(kinds[low] == sub + bf16(first - types * low), counts[low], empty)
        if high != low and high < len(rows):
            group = jnp.where(
                kinds[high] == sub + bf16(first - types * high), counts[high], group
            )
        groups.append(group)
    return jnp.concatenate(groups, axis=0)


def tap_rows(planes_ref, rows, chan, padded, types):
    plane_cells = rows[0].shape[1]
    half_cells = plane_cells // 2
    planes_ref[...] = jnp.zeros_like(planes_ref)
    for x, row in enumerate(rows):
        planes_ref[x:x + 1, LANES:LANES + plane_cells] = row
    start = pl.multiple_of(chan * half_cells, LANES)
    cells = planes_ref[:, pl.ds(start, half_cells + 3 * LANES)]
    column = lax.rem(lax.broadcasted_iota(jnp.int32, (8, padded), 1), SIDE)
    plain, split = [], []
    for shift_y, shift_z in TAPS:
        first = LANES - SIDE + SIDE * shift_y + shift_z
        moved = cells[:, first:first + padded]
        inside = (column + shift_z >= 0) & (column + shift_z < SIDE)
        moved = jnp.where(inside, moved, 0)
        kind = lax.shift_right_logical(moved, 2)
        count = moved & 3
        plain.append((kind.astype(f32), count.astype(f32)))
        split.append(
            (
                jnp.where(count == 3, kind + types, kind).astype(f32),
                jnp.where(count == 3, 1, count).astype(f32),
            )
        )
    return plain, split


def both_hot(plain, split, x, types, first):
    return jnp.concatenate(
        [one_hot(plain, x, types, first), one_hot(split, x, 2 * types, first)], axis=0
    ).T


def hidden_rows(operands, bias1, folded_ref, first, size, half_cells, chan, plane_ok):
    total = bias1
    for dx in range(3):
        total = total + jnp.dot(
            operands[dx](first, size), folded_ref[dx], preferred_element_type=f32
        )
    index = first + lax.broadcasted_iota(jnp.int32, (size, 1), 0)
    lowest = jnp.where(plane_ok, jnp.where(chan == 0, SIDE, 0), half_cells + 2 * SIDE)
    highest = jnp.where(chan == 0, half_cells + 2 * SIDE, half_cells + SIDE)
    inside = (index >= lowest) & (index < highest)
    return jnp.where(inside, jnp.maximum(total, 0.0), 0.0).astype(bf16)


def reader(ref, x):
    return lambda first, size: ref[x, first:first + size, :]


def score_kernel(
    pose_total,
    types,
    own_ref,
    near_ref,
    far_ref,
    head_own_ref,
    head_far_ref,
    folded_ref,
    bias1_ref,
    weight2_ref,
    bias2_ref,
    out_ref,
    planes_ref,
    hot_ref,
    hidden_ref,
    sums_ref,
    head_ref,
):
    chan = lax.axis_index("chan")
    block = lax.axis_index("pose") // pose_total
    plane_cells = own_ref.shape[1]
    half_cells = plane_cells // 2
    padded = hot_ref.shape[1]
    used = half_cells + 2 * SIDE
    share = head_own_ref.shape[0]
    head_cells = pl.ds(pl.multiple_of(chan * half_cells, LANES), half_cells)
    head_ref[pl.ds(pl.multiple_of(chan * share, share), share), :] = head_own_ref[:, head_cells]
    head_ref[pl.ds(pl.multiple_of((1 - chan) * share, share), share), :] = head_far_ref[
        :, head_cells
    ]
    near, far = near_ref[...], far_ref[...]
    sides = []
    for step in (1, 2):
        cells = slice((step - 1) * plane_cells, step * plane_cells)
        end = (block < step) | (block >= XPLANES - step)
        above = (chan == lax.rem(block // step, 2)) != end
        sides.append(
            (
                jnp.where(block >= step, jnp.where(above, far[:, cells], near[:, cells]), 0),
                jnp.where(
                    block < XPLANES - step, jnp.where(above, near[:, cells], far[:, cells]), 0
                ),
            )
        )
    rows = [sides[1][0], sides[0][0], own_ref[...], sides[0][1], sides[1][1]]
    plain, split = tap_rows(planes_ref, rows, chan, padded, types)
    bias1 = bias1_ref[...]
    operands = [reader(hot_ref, x) for x in range(5)]
    plane_ok = [block >= 1, True, block <= XPLANES - 2]
    for first in range(0, padded, TILE):
        size = min(TILE, used - first)
        for x in range(5):
            hot_ref[x, first:first + TILE, :] = both_hot(plain, split, x, types, first)
            if x >= 2:
                h = x - 2
                hidden_ref[h, first:first + size, :] = hidden_rows(
                    operands[h:], bias1, folded_ref, first, size, half_cells, chan, plane_ok[h]
                )

    width = weight2_ref.shape[2]
    hidden = [reader(hidden_ref, h) for h in range(3)]

    def taps(first, size, *numbers):
        total = None
        for h in range(3):
            weights = [weight2_ref[h * 9 + tap] for tap in numbers]
            part = jnp.dot(
                hidden[h](first, size),
                jnp.concatenate(weights, axis=1),
                preferred_element_type=f32,
            )
            total = part if total is None else total + part
        return [total[:, n * width:(n + 1) * width] for n in range(len(numbers))]

    bias2 = bias2_ref[...]
    step = STEP
    column = lax.rem(lax.broadcasted_iota(jnp.int32, (step, 1), 0), SIDE)
    running = jnp.zeros((8, width), f32)
    for first in range(0, half_cells, step):
        tap0, tap1 = taps(first, step, 0, 1)
        tap2, tap3 = taps(first, step + SIDE, 2, 3)
        tap4, tap5 = taps(first + SIDE, step, 4, 5)
        tap6, tap7 = taps(first + 2 * SIDE, step, 6, 7)
        (tap8,) = taps(first + 2 * SIDE, step, 8)
        sums_ref[0, 8 + first:8 + first + step, :] = tap0 + tap3[SIDE:] + tap6
        middle = bias2 + tap1 + tap4 + tap7
        sums_ref[1, 8 + first:8 + first + step, :] = tap2[:step] + tap5 + tap8
        mapped = (
            middle
            + jnp.where(column > 0, sums_ref[0, 7 + first:7 + first + step, :], 0.0)
            + jnp.where(column < SIDE - 1, sums_ref[1, 9 + first:9 + first + step, :], 0.0)
        )
        scored = jnp.maximum(mapped, 0.0) * head_ref[:, first:first + step].T
        running = running + jnp.sum(scored.reshape(step // 8, 8, width), axis=0)
    out_ref[...] = jnp.broadcast_to(jnp.sum(running), out_ref.shape)


def score(types, pose_total, own, near, far, head_own, head_far, folded, bias1, weight2, bias2, copies):
    plane_cells = own.shape[1]
    depth, mid = folded.shape[1:]
    width = weight2.shape[2]
    padded = round_up(plane_cells // 2 + 2 * SIDE, TILE)
    return pl.pallas_call(
        functools.partial(score_kernel, pose_total, types),
        out_shape=pltpu.VMEM((copies, LANES), f32),
        scratch_shapes=[
            pltpu.VMEM((8, plane_cells + 3 * LANES), jnp.int32),
            pltpu.VMEM((5, padded, depth), bf16),
            pltpu.VMEM((3, padded, mid), bf16),
            pltpu.VMEM((2, plane_cells // 2 + 16, width), f32),
            pltpu.VMEM((width, plane_cells // 2), f32),
        ],
        compiler_params=params(40),
        name="score",
    )(
        in_vmem(own),
        in_vmem(near),
        in_vmem(far),
        in_vmem(head_own),
        in_vmem(head_far),
        in_vmem(folded),
        in_vmem(bias1),
        in_vmem(weight2),
        in_vmem(bias2),
    )


def final_kernel(pose_total, chan_count, parts_ref, plane_ref, scores_ref):
    parts = parts_ref[:, 0, :]
    pose = lax.broadcasted_iota(jnp.int32, parts.shape, 0) // chan_count
    first = lax.broadcasted_iota(jnp.int32, parts.shape, 1) == 0
    plane_ref[0] = jnp.sum(jnp.where(first & (pose == lax.axis_index("pose")), parts, 0.0))
    for p in range(pose_total):
        scores_ref[p] = jnp.sum(jnp.where(first & (lax.rem(pose, pose_total) == p), parts, 0.0))


def final_sums(parts, pose_total, chan_count):
    smem = pl.BlockSpec(memory_space=pltpu.SMEM)
    return pl.pallas_call(
        functools.partial(final_kernel, pose_total, chan_count),
        out_shape=(
            jax.ShapeDtypeStruct((1,), f32),
            jax.ShapeDtypeStruct((pose_total,), f32),
        ),
        out_specs=(smem, smem),
        compiler_params=params(1),
        name="final_sums",
    )(in_vmem(parts))


def on_device(
    atom_type,
    occupancy,
    atom_embed,
    conv1_weight,
    conv1_bias,
    conv2_weight,
    conv2_bias,
    head_weight,
):
    chan_count = lax.axis_size("chan")
    pose_count = lax.axis_size("pose")
    pose_total = pose_count // XPLANES
    swap = [(0, 1), (1, 0)]

    def fetch(step):
        pairs = []
        for i in range(pose_count):
            above = i // pose_total // step % 2
            sources = {}
            for core, other in ((above, i + step * pose_total), (1 - above, i - step * pose_total)):
                if 0 <= other < pose_count:
                    sources[core] = 2 * other + core
            for core in (0, 1):
                if core not in sources:
                    sources[core], sources[1 - core] = sources[1 - core], 2 * i + core
            pairs += [(sources[core], 2 * i + core) for core in (0, 1)]
        return lax.ppermute(code, ("pose", "chan"), pairs)

    types = atom_embed.shape[0]
    code = encode(atom_type, occupancy)
    second, first, folded = lax.optimization_barrier(
        (fetch(2), fetch(1), fold_embedding(atom_embed, conv1_weight))
    )
    near = jnp.concatenate([first, second], axis=1)
    far = lax.ppermute(near, "chan", swap)
    head_far = lax.ppermute(head_weight, "chan", swap)
    part = score(
        types,
        pose_total,
        code,
        near,
        far,
        head_weight,
        head_far,
        folded,
        conv1_bias[None, :],
        conv2_weight,
        conv2_bias[None, :],
        pose_count * chan_count,
    )
    parts = lax.all_to_all(part[:, None, :], ("pose", "chan"), 0, 0, tiled=True)
    return final_sums(parts, pose_total, chan_count)


def solution(mesh):
    return jax.shard_map(
        on_device,
        mesh=mesh,
        in_specs=(P("pose", None), P("pose", None), P(), P(), P(), P(), P(), P("chan", None)),
        out_specs=(P("pose"), P()),
        check_vma=False,
    )
```
